32 devices in a mesh: head: 4 (over y, core), ctx: 8 (over z, x).
Axes of the slice: x: 2, y: 2, z: 4, core: 2. Of those that a mesh axis runs over, the one named last changes fastest.
Arguments:
- queries: bfloat16 [6144, 4, 1024], P('ctx', 'head'), may hold values from -200 to 200
- keys: bfloat16 [6144, 4, 128], P('ctx', 'head'), may hold values from -6 to 6
- values: bfloat16 [6144, 4, 128], P('ctx', 'head'), may hold values from -6 to 6
- span_ids: int32 [16], replicated, may hold values from 0 to 15, as said below
Outputs:
- attn_out: bfloat16 [6144, 4, 1024], P('ctx', 'head')
The draws below stay inside these ranges and needn't reach their ends.
Inputs may be any that keep to these rules, and one draw needn't show every extreme that they name: `span_ids`: entry 2r is below 8, entry 2r + 1 equals 15 minus entry 2r, and all entries differ.
All inputs are finite; a program needn't handle non-finite values.
Results may differ from the reference program's by a relative error of at most 0.0055.
Values may be sent and summed in bfloat16 or wider, within the bound.
A program may use at most 64 MiB of HBM per device.

```python
import jax
import jax.numpy as jnp
from jax import lax

HD = 128
GRP = 8
KVH = 4
CH = 384
NCHUNK = 16
TOKENS = 6144
N_CTX = 8


def drawn(key):
    base_keys = jnp.clip(jax.random.normal(jax.random.fold_in(key, 11), (TOKENS, KVH, HD), jnp.float32), -6.0, 6.0)
    return base_keys


def draw_keys(key, part):
    base_keys = drawn(key)
    return base_keys.astype(jnp.bfloat16)


def draw_queries(key, part):
    base = jnp.clip(jax.random.normal(jax.random.fold_in(key, 21), (TOKENS, KVH, GRP * HD), jnp.float32), -6.0, 6.0)
    return base.astype(jnp.bfloat16)


def draw_span_ids(key, part):
    order = jax.random.permutation(jax.random.fold_in(key, 31), N_CTX).astype(jnp.int32)
    return jnp.stack([order, NCHUNK - 1 - order], axis=1).reshape(NCHUNK).astype(jnp.int32)


def block_scale(rng, shape, pieces, low, high):
    def one(position, blocks):
        heights = jax.random.uniform(jax.random.fold_in(jax.random.fold_in(rng, 6), position), (blocks,), jnp.float32, low / len(pieces), high / len(pieces))
        return jnp.repeat(jnp.exp(heights), shape[position] // blocks).reshape((-1,) + (1,) * (len(shape) - position - 1))

    factor_of = one(*pieces[0])
    for cut in pieces[1:]:
        factor_of = factor_of * one(*cut)
    return factor_of


def normal_values(own_key, shape, deviation, most, pieces=(), kind=jnp.bfloat16):
    drawn = deviation * jax.random.normal(own_key, shape, jnp.float32)
    if pieces:
        drawn = drawn * block_scale(own_key, shape, pieces, -0.22, 0.18)
    return jnp.clip(drawn, -most, most).astype(kind)


def setup_inputs(seed: int = 0) -> dict:
    key_of = jax.random.split(jax.random.key(seed), 5)
    return {
        "queries": draw_queries(jax.random.fold_in(key_of[4], 71), 0),
        "keys": draw_keys(jax.random.fold_in(key_of[4], 71), 0),
        "values": normal_values(key_of[2], (TOKENS, KVH, HD), 1.0, 6.0, ((0, 8), (1, 4))),
        "span_ids": draw_span_ids(jax.random.fold_in(key_of[4], 71), 0),
    }


def reference(queries, keys, values, span_ids):
    tokens = queries.shape[0]
    row_ids = jnp.arange(tokens, dtype=jnp.int32)
    positions = (jnp.take(span_ids, row_ids // CH) * CH + row_ids % CH).astype(jnp.int32)
    score_scale = HD ** -0.5
    query_all = jnp.moveaxis(queries.reshape(tokens, KVH, GRP, HD), 1, 0)
    key_all = jnp.moveaxis(keys, 1, 0)
    value_all = jnp.moveaxis(values, 1, 0)

    def one_head(inputs_now):
        query_head, key_head, value_head = inputs_now
        key_float = key_head.astype(jnp.float32)
        value_float = value_head.astype(jnp.float32)
        query_blocks = query_head.reshape(tokens // CH, CH, GRP, HD)
        block_pos = positions.reshape(tokens // CH, CH)

        def one_block(block_now):
            query_block, query_pos = block_now
            scores = jnp.einsum("qgd,kd->qgk", query_block.astype(jnp.float32), key_float,
                                precision=lax.Precision.HIGHEST) * score_scale
            allowed = positions[None, None, :] <= query_pos[:, None, None]
            scores = jnp.where(allowed, scores, -1e30)
            row_max = jnp.max(scores, axis=2, keepdims=True)
            weights = jnp.where(allowed, jnp.exp(scores - row_max), 0.0)
            weight_sum = jnp.sum(weights, axis=2)
            rounded = lax.optimization_barrier(weights.astype(jnp.bfloat16)).astype(jnp.float32)
            mixed = jnp.einsum("qgk,kd->qgd", rounded, value_float, precision=lax.Precision.HIGHEST)
            return (mixed / weight_sum[:, :, None]).astype(jnp.bfloat16)

        return lax.map(one_block, (query_blocks, block_pos)).reshape(tokens, GRP * HD)

    result = lax.map(one_head, (query_all, key_all, value_all))
    return jnp.moveaxis(result, 0, 1)
```

```python
import functools
import math

import jax
import jax.numpy as jnp
from jax import lax
from jax.experimental import pallas as pl
from jax.experimental.pallas import tpu as pltpu
from jax.sharding import PartitionSpec as P

MESH = pl.DeviceIdType.MESH
LOW, HIGH = 0, 1
TO_PARTNER, TO_NEXT, TO_PREV = 0, 1, 2
MASKED = -1e30
TILE = 512
ONES = 16
EMPTY, HIGH_ON_LOW, OWN_LOW, OWN_HIGH, REMOTE = 0, 1, 2, 3, 4


def kernel(
    count, head_dim, ids, q_hbm, k_hbm, v_hbm, o_hbm,
    q_in, q, kv, acc, top, total, s_even, s_odd, p_even, p_odd, out,
    in_sem, out_sem, send_sem, recv_sem,
):
    _, wide, lanes = q_in.shape
    rows = out.shape[1]
    groups = wide * 2 // rows
    span = rows // 2
    line = count // 2
    width = s_even.shape[1]
    tiles = wide // width
    sub = top.shape[1]
    scale = head_dim ** (-0.5) * math.log2(math.e)
    me = lax.axis_index("ctx")
    z = me // 2
    x = me % 2
    partner = z * 2 + 1 - x
    first, last = 1 - x, (line - 1) * 2 + 1 - x

    def kv_in(half, which, src):
        return pltpu.make_async_copy(
            src.at[pl.ds(half * span, span), :], kv.at[me, half, which], in_sem.at[half, which]
        )

    def q_copy(group, half):
        return pltpu.make_async_copy(
            q_hbm.at[pl.ds(half * span, span), pl.ds(group * lanes, lanes)],
            q_in.at[half, pl.ds(group * span, span), :],
            in_sem.at[2 + group, half],
        )

    for half in range(2):
        kv_in(half, 0, k_hbm).start()
        kv_in(half, 1, v_hbm).start()
    for half in range(2):
        for group in range(groups):
            q_copy(group, half).start()

    barrier = pltpu.get_barrier_semaphore()
    pl.semaphore_signal(barrier, inc=1, device_id={"ctx": partner}, device_id_type=MESH)

    @pl.when(z > 0)
    def _():
        pl.semaphore_signal(barrier, inc=1, device_id={"ctx": me - 2}, device_id_type=MESH)

    @pl.when(z < line - 1)
    def _():
        pl.semaphore_signal(barrier, inc=1, device_id={"ctx": me + 2}, device_id_type=MESH)

    near = 1 + jnp.where(z > 0, 1, 0) + jnp.where(z < line - 1, 1, 0)
    pl.semaphore_wait(barrier, near)

    def sent(owner, half, way):
        target = (partner, me + 2, me - 2)[way]
        return pltpu.make_async_remote_copy(
            src_ref=kv.at[owner, half],
            dst_ref=kv.at[owner, half],
            send_sem=send_sem.at[owner, half, way],
            recv_sem=recv_sem.at[owner, half],
            device_id={"ctx": target},
            device_id_type=MESH,
        )

    for half in range(2):
        kv_in(half, 0, k_hbm).wait()
        kv_in(half, 1, v_hbm).wait()

        @pl.when(z < line - 1)
        def _():
            sent(me, half, TO_NEXT).start()

        @pl.when(z > 0)
        def _():
            sent(me, half, TO_PREV).start()

        sent(me, half, TO_PARTNER).start()

    def arrived(owner, half):
        sent(owner, half, TO_PARTNER).wait_recv()

    def crosses(place, half):
        if half == LOW:
            return place >= 0
        by_line = jnp.where(z > 0, jnp.where(place == 0, 1, 0), 0) + jnp.where(
            z < line - 1, jnp.where(place == line - 1, 1, 0), 0
        )
        return by_line == 0

    def relay(step, half):
        before = z - step
        after = z + step

        @pl.when(before >= 0)
        def _():
            owner = before * 2 + x
            arrived(owner, half)

            @pl.when(z < line - 1)
            def _():
                sent(owner, half, TO_NEXT).start()

            @pl.when(crosses(before, half))
            def _():
                sent(owner, half, TO_PARTNER).start()

        @pl.when(after < line)
        def _():
            owner = after * 2 + x
            arrived(owner, half)

            @pl.when(z > 0)
            def _():
                sent(owner, half, TO_PREV).start()

            @pl.when(crosses(after, half))
            def _():
                sent(owner, half, TO_PARTNER).start()

    def pass_on(index):
        @pl.when(index == z)
        def _():
            arrived(first, HIGH)
            sent(first, HIGH, TO_NEXT).start()

        @pl.when(index == line - 1 - z)
        def _():
            arrived(last, HIGH)
            sent(last, HIGH, TO_PREV).start()

    def split_q(group, carry):
        place = pl.ds(pl.multiple_of(group * span, span), span)
        for half in range(2):
            scaled = q_in[half, place, :].astype(jnp.float32) * scale
            coarse = scaled.astype(jnp.bfloat16)
            fine = (scaled - coarse.astype(jnp.float32)).astype(jnp.bfloat16)
            q[half, place, :] = jnp.concatenate([coarse, fine], axis=1)
        return carry

    acc[EMPTY] = jnp.zeros((lanes, wide), jnp.float32)
    top[EMPTY] = jnp.full((sub, wide), MASKED, jnp.float32)
    total[EMPTY] = jnp.zeros((sub, wide), jnp.float32)
    for half in range(2):
        for group in range(groups):
            q_copy(group, half).wait()
    lax.fori_loop(0, groups, split_q, 0)

    def job(half, key_part, value_part, source, target, masked=False):
        keys = jnp.concatenate([key_part, key_part], axis=1)
        values = jnp.concatenate(
            [value_part.T, jnp.ones((ONES, span), value_part.dtype)], axis=0
        )

        def cut(tile):
            return slice(tile * width, (tile + 1) * width)

        def score(tile):
            s = lax.dot_general(
                keys, q[half, cut(tile), :], (((1,), (1,)), ((), ())),
                preferred_element_type=jnp.float32,
            )
            if masked:
                key_no = lax.broadcasted_iota(jnp.int32, (span, width), 0)
                row_no = (lax.broadcasted_iota(jnp.int32, (span, width), 1) + tile * width) % span
                s = jnp.where(key_no <= row_no, s, MASKED)
            (s_even, s_odd)[tile % 2][...] = s
            best = s[:sub]
            for piece in range(1, span // sub):
                best = jnp.maximum(best, s[piece * sub : (piece + 1) * sub])
            old = top[source, :, cut(tile)]
            m = jnp.maximum(old, jnp.max(best, axis=0, keepdims=True))
            top[target, :, cut(tile)] = m
            return m, jnp.exp2(old - m)

        def weigh(tile, m):
            s = (s_even, s_odd)[tile % 2]
            p = (p_even, p_odd)[tile % 2]
            for piece in range(0, span, 2 * sub):
                parts = [
                    jnp.exp2(s[piece + shift : piece + shift + sub] - m) for shift in (0, sub)
                ]
                p[piece : piece + 2 * sub] = jnp.concatenate(parts, axis=0).astype(p.dtype)

        def mix(tile, fade):
            p = (p_even, p_odd)[tile % 2]
            added = jnp.dot(values, p[...], preferred_element_type=jnp.float32)
            spread = jnp.broadcast_to(fade[:1], (lanes, width))
            acc[target, :, cut(tile)] = acc[source, :, cut(tile)] * spread + added[:lanes]
            total[target, :, cut(tile)] = (
                total[source, :, cut(tile)] * fade + added[lanes : lanes + sub]
            )

        state = {}
        for tile in range(-1, tiles + 1):
            if tile + 1 < tiles:
                state[tile + 1] = score(tile + 1)
            if 0 <= tile < tiles:
                weigh(tile, state[tile][0])
            if tile >= 1:
                mix(tile - 1, state[tile - 1][1])

    def own(half, carry):
        job(half, kv[me, half, 0], kv[me, half, 1], EMPTY, OWN_LOW + half, masked=True)
        return carry

    def high_on_low(owner, source):
        job(HIGH, kv[owner, LOW, 0], kv[owner, LOW, 1], source, HIGH_ON_LOW)

    short = jnp.minimum(z, line - 1 - z)
    far_side = jnp.where(z <= line - 1 - z, 1, -1)

    def line_place(order):
        paired = jnp.where(order % 2 == 1, -1, 1) * ((order + 1) // 2)
        alone = far_side * (order - short)
        return z + jnp.where(order <= 2 * short, paired, alone)

    def crossed(order):
        return jnp.where(order == 0, z, line_place(order)) * 2 + 1 - x

    def visited(index, place):
        return jnp.where(place == 0, crossed(index), line_place(index + 1) * 2 + x)

    def is_higher(owner):
        return jnp.where(ids[2 * owner] > ids[2 * me], 1, 0)

    def chain_ends(until):
        low_end, high_end = OWN_LOW, OWN_HIGH
        for turn in range(count - 1):
            flag = is_higher(visited(turn // 2, turn % 2))
            counts = jnp.where(turn < until, 1, 0)
            low_end = jnp.where(counts * (1 - flag) == 1, REMOTE + turn, low_end)
            high_end = jnp.where(counts * flag == 1, REMOTE + turn, high_end)
        return low_end, high_end

    def same_half(owner, turn):
        flag = is_higher(owner)
        is_high = jnp.full((span, lanes), flag, jnp.int32) == 1
        key_part, value_part = [
            jnp.where(is_high, kv[owner, HIGH, which], kv[owner, LOW, which]) for which in range(2)
        ]
        low_end, high_end = chain_ends(turn)
        job(flag, key_part, value_part, jnp.where(flag == 1, high_end, low_end), REMOTE + turn)

    lax.fori_loop(0, 2, own, 0)

    def visit(index, carry):
        across = jnp.where(index < 0, me, crossed(jnp.maximum(index, 0)))
        along = line_place(index + 1) * 2 + x
        some = jnp.logical_and(index >= 0, index < line - 1)
        both = jnp.where(some, 2, 1)

        @pl.when(some)
        def _():
            relay(index + 1, LOW)

        @pl.when(index >= 0)
        def _():
            arrived(across, LOW)

        def low_one(place, carry):
            owner = jnp.where(place == 0, across, along)
            high_on_low(owner, jnp.where(index < 0, EMPTY, HIGH_ON_LOW))
            return carry

        lax.fori_loop(0, both, low_one, 0)

        @pl.when(some)
        def _():
            relay(index + 1, HIGH)
            pass_on(index)

        @pl.when(index >= 0)
        def _():
            arrived_high(index, across)

        def same_one(place, carry):
            owner = jnp.where(place == 0, across, along)
            same_half(owner, 2 * index + place)
            return carry

        lax.fori_loop(0, jnp.where(index < 0, 0, both), same_one, 0)
        return carry

    def arrived_high(index, across):
        from_first = jnp.where(z < line - 1, jnp.where(across == first, 1, 0), 0)
        from_last = jnp.where(z > 0, jnp.where(across == last, 1, 0), 0)
        taken = from_first * jnp.where(index >= z, 1, 0) + from_last * jnp.where(
            index >= line - 1 - z, 1, 0
        )

        @pl.when(taken == 0)
        def _():
            arrived(across, HIGH)

    lax.fori_loop(-1, line, visit, 0)
    low_end, high_end = chain_ends(count - 1)

    def finish(group):
        part = slice(group * span, (group + 1) * span)
        weight = 1.0 / total[low_end, :, part]
        mixed = acc[low_end, :, part] * weight[:1]
        out[group, :span, :] = mixed.astype(out.dtype).T
        m = jnp.maximum(top[HIGH_ON_LOW, :, part], top[high_end, :, part])
        fades = [jnp.exp2(top[which, :, part] - m) for which in (HIGH_ON_LOW, high_end)]
        weight = 1.0 / (
            total[HIGH_ON_LOW, :, part] * fades[0] + total[high_end, :, part] * fades[1]
        )
        mixed = acc[HIGH_ON_LOW, :, part] * (fades[0] * weight)[:1]
        mixed = mixed + acc[high_end, :, part] * (fades[1] * weight)[:1]
        out[group, span:, :] = mixed.astype(out.dtype).T

    def result(group):
        return pltpu.make_async_copy(
            out.at[group], o_hbm.at[:, pl.ds(group * lanes, lanes)], out_sem.at[group]
        )

    for group in range(groups):
        finish(group)
        result(group).start()

    def settle(place, carry):
        owner = place * 2 + x
        for half in range(2):
            @pl.when(crosses(place, half))
            def _():
                sent(owner, half, TO_PARTNER).wait_send()

            @pl.when(jnp.logical_and(place <= z, z < line - 1))
            def _():
                sent(owner, half, TO_NEXT).wait_send()

            @pl.when(jnp.logical_and(place >= z, z > 0))
            def _():
                sent(owner, half, TO_PREV).wait_send()

        return carry

    lax.fori_loop(0, line, settle, 0)

    @pl.when(z < line - 1)
    def _():
        sent(first, HIGH, TO_NEXT).wait_send()

    @pl.when(z > 0)
    def _():
        sent(last, HIGH, TO_PREV).wait_send()

    for group in range(groups):
        result(group).wait()


def local(count, queries, keys, values, span_ids):
    rows = queries.shape[0]
    head_dim = keys.shape[2]
    width = queries.shape[2]
    groups = width // head_dim
    span = rows // 2
    wide = groups * span
    tile = math.gcd(wide, TILE)
    states = REMOTE + count - 1
    any_space = pl.BlockSpec(memory_space=pl.ANY)
    out = pl.pallas_call(
        functools.partial(kernel, count, head_dim),
        out_shape=jax.ShapeDtypeStruct((rows, width), jnp.bfloat16),
        in_specs=[pl.BlockSpec(memory_space=pltpu.SMEM), any_space, any_space, any_space],
        out_specs=any_space,
        scratch_shapes=[
            pltpu.VMEM((2, wide, head_dim), jnp.bfloat16),
            pltpu.VMEM((2, wide, 2 * head_dim), jnp.bfloat16),
            pltpu.VMEM((count, 2, 2, span, head_dim), jnp.bfloat16),
            pltpu.VMEM((states, head_dim, wide), jnp.float32),
            pltpu.VMEM((states, 8, wide), jnp.float32),
            pltpu.VMEM((states, 8, wide), jnp.float32),
            pltpu.VMEM((span, tile), jnp.float32),
            pltpu.VMEM((span, tile), jnp.float32),
            pltpu.VMEM((span, tile), jnp.bfloat16),
            pltpu.VMEM((span, tile), jnp.bfloat16),
            pltpu.VMEM((groups, rows, head_dim), jnp.bfloat16),
            pltpu.SemaphoreType.DMA((2 + groups, 2)),
            pltpu.SemaphoreType.DMA((groups,)),
            pltpu.SemaphoreType.DMA((count, 2, 3)),
            pltpu.SemaphoreType.DMA((count, 2)),
        ],
        compiler_params=pltpu.CompilerParams(
            collective_id=0, has_side_effects=True, vmem_limit_bytes=56 * 2**20
        ),
    )(
        span_ids,
        queries.reshape(rows, width),
        keys.reshape(rows, head_dim),
        values.reshape(rows, head_dim),
    )
    return out.reshape(rows, 1, width)


def solution(mesh):
    in_specs = (P("ctx", "head", None), P("ctx", "head", None), P("ctx", "head", None), P())
    out_specs = P("ctx", "head", None)
    body = functools.partial(local, mesh.shape["ctx"])
    return jax.shard_map(body, mesh=mesh, in_specs=in_specs, out_specs=out_specs, check_vma=False)
```

```python
import functools
import math

import jax
import jax.numpy as jnp
from jax import lax
from jax.experimental import pallas as pl
from jax.experimental.pallas import tpu as pltpu
from jax.sharding import PartitionSpec as P

MESH = pl.DeviceIdType.MESH
LOW, HIGH = 0, 1
PIECES = 2
TO_PARTNER, TO_NEXT, TO_PREV = 0, 1, 2
MASKED = -1e30
TILE = 512
ONES = 16
EMPTY, HIGH_ON_LOW, OWN_LOW, OWN_HIGH, REMOTE = 0, 1, 2, 3, 4


def kernel(
    count, head_dim, ids, q_hbm, k_hbm, v_hbm, out,
    q_in, q, kv, acc, top, total, s_even, s_odd, p_even, p_odd,
    kv_sem, in_sem, send_sem, recv_sem,
):
    _, wide, lanes = q_in.shape
    rows = out.shape[0]
    groups = wide * 2 // rows
    span = rows // 2
    line = count // 2
    width = s_even.shape[1]
    tiles = wide // width
    sub = top.shape[1]
    scale = head_dim ** (-0.5) * math.log2(math.e)
    me = lax.axis_index("ctx")
    z = me // 2
    x = me % 2
    partner = z * 2 + 1 - x
    first, last = 1 - x, (line - 1) * 2 + 1 - x
    near_end = jnp.where(z <= line - 1 - z, -1, 1)

    short_span = span // PIECES

    def kv_in(half, piece, which):
        return pltpu.make_async_copy(
            (k_hbm, v_hbm)[which].at[pl.ds(half * span + piece * short_span, short_span), :],
            kv.at[me, half, piece, which],
            kv_sem.at[half, piece, which],
        )

    def q_copy(group, half):
        return pltpu.make_async_copy(
            q_hbm.at[pl.ds(half * span, span), pl.ds(group * lanes, lanes)],
            q_in.at[half, pl.ds(group * span, span), :],
            in_sem.at[group, half],
        )

    for half in range(2):
        for piece in range(PIECES):
            for which in range(2):
                kv_in(half, piece, which).start()
    for half in range(2):
        for group in range(groups):
            q_copy(group, half).start()

    barrier = pltpu.get_barrier_semaphore()
    pl.semaphore_signal(barrier, inc=1, device_id={"ctx": partner}, device_id_type=MESH)

    @pl.when(z > 0)
    def _():
        pl.semaphore_signal(barrier, inc=1, device_id={"ctx": me - 2}, device_id_type=MESH)

    @pl.when(z < line - 1)
    def _():
        pl.semaphore_signal(barrier, inc=1, device_id={"ctx": me + 2}, device_id_type=MESH)

    near = 1 + jnp.where(z > 0, 1, 0) + jnp.where(z < line - 1, 1, 0)
    pl.semaphore_wait(barrier, near)

    def piece_sent(owner, half, piece, way):
        along = jnp.where(way == TO_NEXT, me + 2, me - 2)
        target = jnp.where(way == TO_PARTNER, partner, along)
        return pltpu.make_async_remote_copy(
            src_ref=kv.at[owner, half, piece],
            dst_ref=kv.at[owner, half, piece],
            send_sem=send_sem.at[owner, half, piece, way],
            recv_sem=recv_sem.at[owner, half, piece],
            device_id={"ctx": target},
            device_id_type=MESH,
        )

    class Sent:
        def __init__(self, owner, half, way):
            self.copies = [piece_sent(owner, half, piece, way) for piece in range(PIECES)]

        def start(self):
            for copy in self.copies:
                copy.start()

        def wait_send(self):
            for copy in self.copies:
                copy.wait_send()

        def wait_recv(self):
            for copy in self.copies:
                copy.wait_recv()

    sent = Sent

    for half in range(2):
        for piece in range(PIECES):
            for which in range(2):
                kv_in(half, piece, which).wait()

            @pl.when(z < line - 1)
            def _():
                piece_sent(me, half, piece, TO_NEXT).start()

            @pl.when(z > 0)
            def _():
                piece_sent(me, half, piece, TO_PREV).start()

            piece_sent(me, half, piece, TO_PARTNER).start()

    def arrived(owner, half, pieces=range(PIECES)):
        for piece in pieces:
            piece_sent(owner, half, piece, TO_PARTNER).wait_recv()

    def crosses(place, half):
        if half == LOW:
            return place >= 0
        by_line = jnp.where(z > 0, jnp.where(place == 0, 1, 0), 0) + jnp.where(
            z < line - 1, jnp.where(place == line - 1, 1, 0), 0
        )
        return by_line == 0

    def relay(step, half):
        for place in (z + near_end * step, z - near_end * step):
            inside = jnp.where(place >= 0, 1, 0) * jnp.where(place < line, 1, 0)
            onward = jnp.where(place < z, jnp.where(z < line - 1, 1, 0), jnp.where(z > 0, 1, 0))
            owner = place * 2 + x

            @pl.when(inside == 1)
            def _():
                arrived(owner, half)

            @pl.when(inside * onward == 1)
            def _():
                sent(owner, half, jnp.where(place < z, TO_NEXT, TO_PREV)).start()

            @pl.when(jnp.logical_and(inside == 1, crosses(place, half)))
            def _():
                sent(owner, half, TO_PARTNER).start()

    def pass_on(index):
        @pl.when(index == z)
        def _():
            arrived(first, HIGH)
            sent(first, HIGH, TO_NEXT).start()

        @pl.when(index == line - 1 - z)
        def _():
            arrived(last, HIGH)
            sent(last, HIGH, TO_PREV).start()

    def split_q(group, carry):
        place = pl.ds(pl.multiple_of(group * span, span), span)
        for half in range(2):
            scaled = q_in[half, place, :].astype(jnp.float32) * scale
            coarse = scaled.astype(jnp.bfloat16)
            fine = (scaled - coarse.astype(jnp.float32)).astype(jnp.bfloat16)
            q[half, place, :] = jnp.concatenate([coarse, fine], axis=1)
        return carry

    acc[EMPTY] = jnp.zeros((lanes, wide), jnp.float32)
    top[EMPTY] = jnp.full((sub, wide), MASKED, jnp.float32)
    total[EMPTY] = jnp.zeros((sub, wide), jnp.float32)
    for half in range(2):
        for group in range(groups):
            q_copy(group, half).wait()
    lax.fori_loop(0, groups, split_q, 0)

    def cut(tile):
        return slice(tile * width, (tile + 1) * width)

    class Job:
        def __init__(self, half, key_parts, value_parts, source, target, masked=False):
            self.half, self.source, self.target, self.masked = half, source, target, masked
            keys = jnp.concatenate(key_parts, axis=0)
            self.keys = jnp.concatenate([keys, keys], axis=1)
            self.length = keys.shape[0]
            values = jnp.concatenate([part.T for part in value_parts], axis=1)
            self.values = jnp.concatenate(
                [values, jnp.ones((ONES, self.length), values.dtype)], axis=0
            )

        def score(self, tile, s_ref):
            s = lax.dot_general(
                self.keys, q[self.half, cut(tile), :], (((1,), (1,)), ((), ())),
                preferred_element_type=jnp.float32,
            )
            if self.masked:
                s = jnp.concatenate(
                    [self.causal(s, tile, place) for place in range(0, width, lanes)], axis=1
                )
            s_ref[: self.length] = s
            best = s[:sub]
            for piece in range(1, self.length // sub):
                best = jnp.maximum(best, s[piece * sub : (piece + 1) * sub])
            old = top[self.source, :, cut(tile)]
            m = jnp.maximum(old, jnp.max(best, axis=0, keepdims=True))
            top[self.target, :, cut(tile)] = m
            return m, jnp.exp2(old - m)

        def causal(self, s, tile, place):
            first_row = (tile * width + place) % span
            blocks = []
            for first_key in range(0, span, lanes):
                block = s[first_key : first_key + lanes, place : place + lanes]
                if first_key > first_row:
                    block = jnp.full_like(block, MASKED)
                elif first_key == first_row:
                    key_no = lax.broadcasted_iota(jnp.int32, block.shape, 0)
                    row_no = lax.broadcasted_iota(jnp.int32, block.shape, 1)
                    block = jnp.where(key_no <= row_no, block, MASKED)
                blocks.append(block)
            return jnp.concatenate(blocks, axis=0)

        def weigh(self, m, s, p):
            for piece in range(0, self.length, 2 * sub):
                parts = [
                    jnp.exp2(s[piece + shift : piece + shift + sub] - m) for shift in (0, sub)
                ]
                p[piece : piece + 2 * sub] = jnp.concatenate(parts, axis=0).astype(p.dtype)

        def mix(self, tile, fade, p):
            added = jnp.dot(self.values, p[: self.length], preferred_element_type=jnp.float32)
            spread = jnp.broadcast_to(fade[:1], (lanes, width))
            acc[self.target, :, cut(tile)] = (
                acc[self.source, :, cut(tile)] * spread + added[:lanes]
            )
            total[self.target, :, cut(tile)] = (
                total[self.source, :, cut(tile)] * fade + added[lanes : lanes + sub]
            )

    def run(*jobs):
        steps = [(job, tile) for job in jobs for tile in range(tiles)]
        scores, shares = (s_even, s_odd), (p_even, p_odd)
        state = {}
        for at in range(-1, len(steps) + 1):
            if at + 1 < len(steps):
                job, tile = steps[at + 1]
                state[at + 1] = job.score(tile, scores[(at + 1) % 2])
            if 0 <= at < len(steps):
                steps[at][0].weigh(state[at][0], scores[at % 2], shares[at % 2])
            if at >= 1:
                job, tile = steps[at - 1]
                job.mix(tile, state[at - 1][1], shares[(at - 1) % 2])

    every = tuple(range(PIECES))

    def parts(owner, half, which, pieces=every):
        return [kv[owner, half, piece, which] for piece in pieces]

    def own_job(half):
        return Job(
            half, parts(me, half, 0), parts(me, half, 1), EMPTY, OWN_LOW + half, masked=True
        )

    def low_job(owners, source, pieces=every):
        return Job(
            HIGH,
            [part for owner in owners for part in parts(owner, LOW, 0, pieces)],
            [part for owner in owners for part in parts(owner, LOW, 1, pieces)],
            source, HIGH_ON_LOW,
        )

    short = jnp.minimum(z, line - 1 - z)

    def line_place(order):
        paired = jnp.where(order % 2 == 1, 1, -1) * ((order + 1) // 2)
        alone = short - order
        return z + near_end * jnp.where(order <= 2 * short, paired, alone)

    def crossed(order):
        return jnp.where(order == 0, z, line_place(order)) * 2 + 1 - x

    def visited(index, place):
        return jnp.where(place == 0, crossed(index), line_place(index + 1) * 2 + x)

    def is_higher(owner):
        return jnp.where(ids[2 * owner] > ids[2 * me], 1, 0)

    def chain_ends(until):
        low_end, high_end = OWN_LOW, OWN_HIGH
        for turn in range(count - 1):
            flag = is_higher(visited(turn // 2, turn % 2))
            counts = jnp.where(turn < until, 1, 0)
            low_end = jnp.where(counts * (1 - flag) == 1, REMOTE + turn, low_end)
            high_end = jnp.where(counts * flag == 1, REMOTE + turn, high_end)
        return low_end, high_end

    def same_job(owner, turn, pieces=every, again=False):
        flag = is_higher(owner)
        is_high = jnp.full((short_span, lanes), flag, jnp.int32) == 1
        key_parts, value_parts = [
            [
                jnp.where(is_high, high, low)
                for high, low in zip(
                    parts(owner, HIGH, which, pieces), parts(owner, LOW, which, pieces)
                )
            ]
            for which in range(2)
        ]
        low_end, high_end = chain_ends(turn)
        source = REMOTE + turn if again else jnp.where(flag == 1, high_end, low_end)
        return Job(flag, key_parts, value_parts, source, REMOTE + turn)

    run(own_job(LOW), own_job(HIGH), low_job([me], EMPTY))

    def visit(index, carry):
        across, along = visited(index, 0), visited(index, 1)
        relay(index + 1, LOW)
        arrived(across, LOW)
        run(low_job([across, along], HIGH_ON_LOW))
        relay(index + 1, HIGH)
        pass_on(index)
        arrived_high(index, across)
        run(same_job(across, 2 * index), same_job(along, 2 * index + 1))
        return carry

    def arrived_high(index, across, pieces=range(PIECES)):
        from_first = jnp.where(z < line - 1, jnp.where(across == first, 1, 0), 0)
        from_last = jnp.where(z > 0, jnp.where(across == last, 1, 0), 0)
        taken = from_first * jnp.where(index >= z, 1, 0) + from_last * jnp.where(
            index >= line - 1 - z, 1, 0
        )

        @pl.when(taken == 0)
        def _():
            arrived(across, HIGH, pieces)

    lax.fori_loop(0, line - 1, visit, 0)
    final = visited(line - 1, 0)
    for piece in range(PIECES):
        arrived(final, LOW, (piece,))
        arrived_high(line - 1, final, (piece,))
        run(
            low_job([final], HIGH_ON_LOW, (piece,)),
            same_job(final, count - 2, (piece,), again=piece > 0),
        )
    low_end, high_end = chain_ends(count - 1)

    def finish(group):
        part = slice(group * span, (group + 1) * span)
        weight = 1.0 / total[low_end, :, part]
        mixed = acc[low_end, :, part] * weight[:1]
        out[:span, group * lanes : (group + 1) * lanes] = mixed.astype(out.dtype).T
        m = jnp.maximum(top[HIGH_ON_LOW, :, part], top[high_end, :, part])
        fades = [jnp.exp2(top[which, :, part] - m) for which in (HIGH_ON_LOW, high_end)]
        weight = 1.0 / (
            total[HIGH_ON_LOW, :, part] * fades[0] + total[high_end, :, part] * fades[1]
        )
        mixed = acc[HIGH_ON_LOW, :, part] * (fades[0] * weight)[:1]
        mixed = mixed + acc[high_end, :, part] * (fades[1] * weight)[:1]
        out[span:, group * lanes : (group + 1) * lanes] = mixed.astype(out.dtype).T

    for group in range(groups):
        finish(group)

    def settle(place, carry):
        owner = place * 2 + x
        for half in range(2):
            @pl.when(crosses(place, half))
            def _():
                sent(owner, half, TO_PARTNER).wait_send()

            @pl.when(jnp.logical_and(place <= z, z < line - 1))
            def _():
                sent(owner, half, TO_NEXT).wait_send()

            @pl.when(jnp.logical_and(place >= z, z > 0))
            def _():
                sent(owner, half, TO_PREV).wait_send()

        return carry

    lax.fori_loop(0, line, settle, 0)

    @pl.when(z < line - 1)
    def _():
        sent(first, HIGH, TO_NEXT).wait_send()

    @pl.when(z > 0)
    def _():
        sent(last, HIGH, TO_PREV).wait_send()


def local(count, queries, keys, values, span_ids):
    rows = queries.shape[0]
    head_dim = keys.shape[2]
    width = queries.shape[2]
    groups = width // head_dim
    span = rows // 2
    wide = groups * span
    tile = math.gcd(wide, TILE)
    states = REMOTE + count - 1
    in_hbm = pl.BlockSpec(memory_space=pltpu.HBM)
    out = pl.pallas_call(
        functools.partial(kernel, count, head_dim),
        out_shape=pltpu.VMEM((rows, width), jnp.bfloat16),
        in_specs=[pl.BlockSpec(memory_space=pltpu.SMEM), in_hbm, in_hbm, in_hbm],
        out_specs=pl.BlockSpec(memory_space=pltpu.VMEM),
        scratch_shapes=[
            pltpu.VMEM((2, wide, head_dim), jnp.bfloat16),
            pltpu.VMEM((2, wide, 2 * head_dim), jnp.bfloat16),
            pltpu.VMEM((count, 2, PIECES, 2, span // PIECES, head_dim), jnp.bfloat16),
            pltpu.VMEM((states, head_dim, wide), jnp.float32),
            pltpu.VMEM((states, 8, wide), jnp.float32),
            pltpu.VMEM((states, 8, wide), jnp.float32),
            pltpu.VMEM((rows, tile), jnp.float32),
            pltpu.VMEM((rows, tile), jnp.float32),
            pltpu.VMEM((rows, tile), jnp.bfloat16),
            pltpu.VMEM((rows, tile), jnp.bfloat16),
            pltpu.SemaphoreType.DMA((2, PIECES, 2)),
            pltpu.SemaphoreType.DMA((groups, 2)),
            pltpu.SemaphoreType.DMA((count, 2, PIECES, 3)),
            pltpu.SemaphoreType.DMA((count, 2, PIECES)),
        ],
        compiler_params=pltpu.CompilerParams(
            collective_id=0, has_side_effects=True, vmem_limit_bytes=60 * 2**20
        ),
    )(
        span_ids,
        queries.reshape(rows, width),
        keys.reshape(rows, head_dim),
        values.reshape(rows, head_dim),
    )
    return out.reshape(rows, 1, width)


def solution(mesh):
    in_specs = (P("ctx", "head", None), P("ctx", "head", None), P("ctx", "head", None), P())
    out_specs = P("ctx", "head", None)
    body = functools.partial(local, mesh.shape["ctx"])
    return jax.shard_map(body, mesh=mesh, in_specs=in_specs, out_specs=out_specs, check_vma=False)
```

```python
import functools
import math

import jax
import jax.numpy as jnp
from jax import lax
from jax.experimental import pallas as pl
from jax.experimental.pallas import tpu as pltpu
from jax.sharding import PartitionSpec as P

MESH = pl.DeviceIdType.MESH
LOW, HIGH = 0, 1
PIECES = 2
TO_PARTNER, TO_NEXT, TO_PREV = 0, 1, 2
MASKED = -1e30
TILE = 768
ONES = 16
EMPTY, HIGH_ON_LOW, OWN_LOW, OWN_HIGH, REMOTE = 0, 1, 2, 3, 4


def kernel(
    count, head_dim, ids, q_hbm, k_hbm, v_hbm, out,
    q_in, q, kv, acc, top, total, s_even, s_odd, p_even, p_odd,
    kv_sem, in_sem, send_sem, recv_sem,
):
    _, wide, lanes = q_in.shape
    rows = out.shape[0]
    groups = wide * 2 // rows
    span = rows // 2
    line = count // 2
    width = s_even.shape[1]
    tiles = wide // width
    sub = top.shape[1]
    scale = head_dim ** (-0.5) * math.log2(math.e)
    me = lax.axis_index("ctx")
    z = me // 2
    x = me % 2
    partner = z * 2 + 1 - x
    first, last = 1 - x, (line - 1) * 2 + 1 - x
    near_end = jnp.where(z <= line - 1 - z, -1, 1)

    short_span = span // PIECES

    def kv_in(half, piece, which):
        return pltpu.make_async_copy(
            (k_hbm, v_hbm)[which].at[pl.ds(half * span + piece * short_span, short_span), :],
            kv.at[me, half, piece, which],
            kv_sem.at[half, piece, which],
        )

    def q_copy(group, half):
        return pltpu.make_async_copy(
            q_hbm.at[pl.ds(half * span, span), pl.ds(group * lanes, lanes)],
            q_in.at[half, pl.ds(group * span, span), :],
            in_sem.at[group, half],
        )

    for half in range(2):
        for piece in range(PIECES):
            for which in range(2):
                kv_in(half, piece, which).start()
    barrier = pltpu.get_barrier_semaphore()
    pl.semaphore_signal(barrier, inc=1, device_id={"ctx": partner}, device_id_type=MESH)

    @pl.when(z > 0)
    def _():
        pl.semaphore_signal(barrier, inc=1, device_id={"ctx": me - 2}, device_id_type=MESH)

    @pl.when(z < line - 1)
    def _():
        pl.semaphore_signal(barrier, inc=1, device_id={"ctx": me + 2}, device_id_type=MESH)

    near = 1 + jnp.where(z > 0, 1, 0) + jnp.where(z < line - 1, 1, 0)
    pl.semaphore_wait(barrier, near)

    def piece_sent(owner, half, piece, way):
        along = jnp.where(way == TO_NEXT, me + 2, me - 2)
        target = jnp.where(way == TO_PARTNER, partner, along)
        return pltpu.make_async_remote_copy(
            src_ref=kv.at[owner, half, piece],
            dst_ref=kv.at[owner, half, piece],
            send_sem=send_sem.at[owner, half, piece, way],
            recv_sem=recv_sem.at[owner, half, piece],
            device_id={"ctx": target},
            device_id_type=MESH,
        )

    class Sent:
        def __init__(self, owner, half, way):
            self.copies = [piece_sent(owner, half, piece, way) for piece in range(PIECES)]

        def start(self):
            for copy in self.copies:
                copy.start()

        def wait_send(self):
            for copy in self.copies:
                copy.wait_send()

        def wait_recv(self):
            for copy in self.copies:
                copy.wait_recv()

    sent = Sent

    for half in range(2):
        for piece in range(PIECES):
            for which in range(2):
                kv_in(half, piece, which).wait()

            @pl.when(z < line - 1)
            def _():
                piece_sent(me, half, piece, TO_NEXT).start()

            @pl.when(z > 0)
            def _():
                piece_sent(me, half, piece, TO_PREV).start()

            piece_sent(me, half, piece, TO_PARTNER).start()

    for half in range(2):
        for group in range(groups):
            q_copy(group, half).start()

    def arrived(owner, half, pieces=range(PIECES)):
        for piece in pieces:
            piece_sent(owner, half, piece, TO_PARTNER).wait_recv()

    def crosses(place, half):
        if half == LOW:
            return place >= 0
        by_line = jnp.where(z > 0, jnp.where(place == 0, 1, 0), 0) + jnp.where(
            z < line - 1, jnp.where(place == line - 1, 1, 0), 0
        )
        return by_line == 0

    def relay(step, half):
        for place in (z + near_end * step, z - near_end * step):
            inside = jnp.where(place >= 0, 1, 0) * jnp.where(place < line, 1, 0)
            onward = jnp.where(place < z, jnp.where(z < line - 1, 1, 0), jnp.where(z > 0, 1, 0))
            owner = place * 2 + x

            @pl.when(inside == 1)
            def _():
                arrived(owner, half)

            @pl.when(inside * onward == 1)
            def _():
                sent(owner, half, jnp.where(place < z, TO_NEXT, TO_PREV)).start()

            @pl.when(jnp.logical_and(inside == 1, crosses(place, half)))
            def _():
                sent(owner, half, TO_PARTNER).start()

    def pass_on(index, at_high):
        upward = jnp.where(z == 0, 1, 0)
        downward = jnp.where(z == line - 1, 1, 0)

        @pl.when(jnp.where(index == z, 1, 0) * jnp.where(upward == at_high, 1, 0) == 1)
        def _():
            arrived(first, HIGH)
            sent(first, HIGH, TO_NEXT).start()

        @pl.when(
            jnp.where(index == line - 1 - z, 1, 0) * jnp.where(downward == at_high, 1, 0) == 1
        )
        def _():
            arrived(last, HIGH)
            sent(last, HIGH, TO_PREV).start()

    def split_q(group, carry):
        place = pl.ds(pl.multiple_of(group * span, span), span)
        for half in range(2):
            scaled = q_in[half, place, :].astype(jnp.float32) * scale
            coarse = scaled.astype(jnp.bfloat16)
            fine = (scaled - coarse.astype(jnp.float32)).astype(jnp.bfloat16)
            q[half, place, :] = jnp.concatenate([coarse, fine], axis=1)
        return carry

    acc[EMPTY] = jnp.zeros((lanes, wide), jnp.float32)
    top[EMPTY] = jnp.full((sub, wide), MASKED, jnp.float32)
    total[EMPTY] = jnp.zeros((sub, wide), jnp.float32)
    for half in range(2):
        for group in range(groups):
            q_copy(group, half).wait()
    lax.fori_loop(0, groups, split_q, 0)

    def cut(tile):
        return slice(tile * width, (tile + 1) * width)

    class Job:
        def __init__(self, half, key_parts, value_parts, source, target, masked=False):
            self.half, self.source, self.target, self.masked = half, source, target, masked
            keys = jnp.concatenate(key_parts, axis=0)
            self.keys = jnp.concatenate([keys, keys], axis=1)
            self.length = keys.shape[0]
            values = jnp.concatenate([part.T for part in value_parts], axis=1)
            self.values = jnp.concatenate(
                [values, jnp.ones((ONES, self.length), values.dtype)], axis=0
            )

        def score(self, tile, s_ref):
            s = lax.dot_general(
                self.keys, q[self.half, cut(tile), :], (((1,), (1,)), ((), ())),
                preferred_element_type=jnp.float32,
            )
            if self.masked:
                s = jnp.concatenate(
                    [self.causal(s, tile, place) for place in range(0, width, lanes)], axis=1
                )
            s_ref[: self.length] = s
            best = s[:sub]
            for piece in range(1, self.length // sub):
                best = jnp.maximum(best, s[piece * sub : (piece + 1) * sub])
            old = top[self.source, :, cut(tile)]
            m = jnp.maximum(old, jnp.max(best, axis=0, keepdims=True))
            top[self.target, :, cut(tile)] = m
            return m, jnp.exp2(old - m)

        def causal(self, s, tile, place):
            first_row = (tile * width + place) % span
            blocks = []
            for first_key in range(0, span, lanes):
                block = s[first_key : first_key + lanes, place : place + lanes]
                if first_key > first_row:
                    block = jnp.full_like(block, MASKED)
                elif first_key == first_row:
                    key_no = lax.broadcasted_iota(jnp.int32, block.shape, 0)
                    row_no = lax.broadcasted_iota(jnp.int32, block.shape, 1)
                    block = jnp.where(key_no <= row_no, block, MASKED)
                blocks.append(block)
            return jnp.concatenate(blocks, axis=0)

        def weigh(self, m, s, p):
            for piece in range(0, self.length, 2 * sub):
                parts = [
                    jnp.exp2(s[piece + shift : piece + shift + sub] - m) for shift in (0, sub)
                ]
                p[piece : piece + 2 * sub] = jnp.concatenate(parts, axis=0).astype(p.dtype)

        def mix(self, tile, fade, p):
            added = jnp.dot(self.values, p[: self.length], preferred_element_type=jnp.float32)
            spread = jnp.broadcast_to(fade[:1], (lanes, width))
            acc[self.target, :, cut(tile)] = (
                acc[self.source, :, cut(tile)] * spread + added[:lanes]
            )
            total[self.target, :, cut(tile)] = (
                total[self.source, :, cut(tile)] * fade + added[lanes : lanes + sub]
            )

    def run(*jobs):
        steps = [(job, tile) for job in jobs for tile in range(tiles)]
        scores, shares = (s_even, s_odd), (p_even, p_odd)
        state = {}
        for at in range(-1, len(steps) + 1):
            if at + 1 < len(steps):
                job, tile = steps[at + 1]
                state[at + 1] = job.score(tile, scores[(at + 1) % 2])
            if 0 <= at < len(steps):
                steps[at][0].weigh(state[at][0], scores[at % 2], shares[at % 2])
            if at >= 1:
                job, tile = steps[at - 1]
                job.mix(tile, state[at - 1][1], shares[(at - 1) % 2])

    every = tuple(range(PIECES))

    def parts(owner, half, which, pieces=every):
        return [kv[owner, half, piece, which] for piece in pieces]

    def own_job(half):
        return Job(
            half, parts(me, half, 0), parts(me, half, 1), EMPTY, OWN_LOW + half, masked=True
        )

    def low_job(owners, source, pieces=every):
        return Job(
            HIGH,
            [part for owner in owners for part in parts(owner, LOW, 0, pieces)],
            [part for owner in owners for part in parts(owner, LOW, 1, pieces)],
            source, HIGH_ON_LOW,
        )

    short = jnp.minimum(z, line - 1 - z)

    def line_place(order):
        paired = jnp.where(order % 2 == 1, 1, -1) * ((order + 1) // 2)
        alone = short - order
        return z + near_end * jnp.where(order <= 2 * short, paired, alone)

    def crossed(order):
        return jnp.where(order == 0, z, line_place(order)) * 2 + 1 - x

    def visited(index, place):
        return jnp.where(place == 0, crossed(index), line_place(index + 1) * 2 + x)

    def is_higher(owner):
        return jnp.where(ids[2 * owner] > ids[2 * me], 1, 0)

    def chain_ends(until):
        low_end, high_end = OWN_LOW, OWN_HIGH
        for turn in range(count - 1):
            flag = is_higher(visited(turn // 2, turn % 2))
            counts = jnp.where(turn < until, 1, 0)
            low_end = jnp.where(counts * (1 - flag) == 1, REMOTE + turn, low_end)
            high_end = jnp.where(counts * flag == 1, REMOTE + turn, high_end)
        return low_end, high_end

    def same_job(owner, turn, pieces=every, again=False):
        flag = is_higher(owner)
        is_high = jnp.full((short_span, lanes), flag, jnp.int32) == 1
        key_parts, value_parts = [
            [
                jnp.where(is_high, high, low)
                for high, low in zip(
                    parts(owner, HIGH, which, pieces), parts(owner, LOW, which, pieces)
                )
            ]
            for which in range(2)
        ]
        low_end, high_end = chain_ends(turn)
        source = REMOTE + turn if again else jnp.where(flag == 1, high_end, low_end)
        return Job(flag, key_parts, value_parts, source, REMOTE + turn)

    run(own_job(LOW), own_job(HIGH), low_job([me], EMPTY))

    def visit(index, carry):
        across, along = visited(index, 0), visited(index, 1)
        relay(index + 1, LOW)
        pass_on(index, 0)
        arrived(across, LOW)
        run(low_job([across, along], HIGH_ON_LOW))
        relay(index + 1, HIGH)
        pass_on(index, 1)
        arrived_high(index, across)
        run(same_job(across, 2 * index), same_job(along, 2 * index + 1))
        return carry

    def arrived_high(index, across, pieces=range(PIECES)):
        from_first = jnp.where(z < line - 1, jnp.where(across == first, 1, 0), 0)
        from_last = jnp.where(z > 0, jnp.where(across == last, 1, 0), 0)
        taken = from_first * jnp.where(index >= z, 1, 0) + from_last * jnp.where(
            index >= line - 1 - z, 1, 0
        )

        @pl.when(taken == 0)
        def _():
            arrived(across, HIGH, pieces)

    lax.fori_loop(0, line - 1, visit, 0)
    final = visited(line - 1, 0)
    for piece in range(PIECES):
        arrived(final, LOW, (piece,))
        arrived_high(line - 1, final, (piece,))
        run(
            low_job([final], HIGH_ON_LOW, (piece,)),
            same_job(final, count - 2, (piece,), again=piece > 0),
        )
    low_end, high_end = chain_ends(count - 1)

    def finish(group):
        part = slice(group * span, (group + 1) * span)
        weight = 1.0 / total[low_end, :, part]
        mixed = acc[low_end, :, part] * weight[:1]
        out[:span, group * lanes : (group + 1) * lanes] = mixed.astype(out.dtype).T
        m = jnp.maximum(top[HIGH_ON_LOW, :, part], top[high_end, :, part])
        fades = [jnp.exp2(top[which, :, part] - m) for which in (HIGH_ON_LOW, high_end)]
        weight = 1.0 / (
            total[HIGH_ON_LOW, :, part] * fades[0] + total[high_end, :, part] * fades[1]
        )
        mixed = acc[HIGH_ON_LOW, :, part] * (fades[0] * weight)[:1]
        mixed = mixed + acc[high_end, :, part] * (fades[1] * weight)[:1]
        out[span:, group * lanes : (group + 1) * lanes] = mixed.astype(out.dtype).T

    for group in range(groups):
        finish(group)

    def settle(place, carry):
        owner = place * 2 + x
        for half in range(2):
            @pl.when(crosses(place, half))
            def _():
                sent(owner, half, TO_PARTNER).wait_send()

            @pl.when(jnp.logical_and(place <= z, z < line - 1))
            def _():
                sent(owner, half, TO_NEXT).wait_send()

            @pl.when(jnp.logical_and(place >= z, z > 0))
            def _():
                sent(owner, half, TO_PREV).wait_send()

        return carry

    lax.fori_loop(0, line, settle, 0)

    @pl.when(z < line - 1)
    def _():
        sent(first, HIGH, TO_NEXT).wait_send()

    @pl.when(z > 0)
    def _():
        sent(last, HIGH, TO_PREV).wait_send()


def local(count, queries, keys, values, span_ids):
    rows = queries.shape[0]
    head_dim = keys.shape[2]
    width = queries.shape[2]
    groups = width // head_dim
    span = rows // 2
    wide = groups * span
    tile = math.gcd(wide, TILE)
    states = REMOTE + count - 1
    in_hbm = pl.BlockSpec(memory_space=pltpu.HBM)
    out = pl.pallas_call(
        functools.partial(kernel, count, head_dim),
        out_shape=pltpu.VMEM((rows, width), jnp.bfloat16),
        in_specs=[pl.BlockSpec(memory_space=pltpu.SMEM), in_hbm, in_hbm, in_hbm],
        out_specs=pl.BlockSpec(memory_space=pltpu.VMEM),
        scratch_shapes=[
            pltpu.VMEM((2, wide, head_dim), jnp.bfloat16),
            pltpu.VMEM((2, wide, 2 * head_dim), jnp.bfloat16),
            pltpu.VMEM((count, 2, PIECES, 2, span // PIECES, head_dim), jnp.bfloat16),
            pltpu.VMEM((states, head_dim, wide), jnp.float32),
            pltpu.VMEM((states, 8, wide), jnp.float32),
            pltpu.VMEM((states, 8, wide), jnp.float32),
            pltpu.VMEM((rows, tile), jnp.float32),
            pltpu.VMEM((rows, tile), jnp.float32),
            pltpu.VMEM((rows, tile), jnp.bfloat16),
            pltpu.VMEM((rows, tile), jnp.bfloat16),
            pltpu.SemaphoreType.DMA((2, PIECES, 2)),
            pltpu.SemaphoreType.DMA((groups, 2)),
            pltpu.SemaphoreType.DMA((count, 2, PIECES, 3)),
            pltpu.SemaphoreType.DMA((count, 2, PIECES)),
        ],
        compiler_params=pltpu.CompilerParams(
            collective_id=0, has_side_effects=True, vmem_limit_bytes=60 * 2**20
        ),
    )(
        span_ids,
        queries.reshape(rows, width),
        keys.reshape(rows, head_dim),
        values.reshape(rows, head_dim),
    )
    return out.reshape(rows, 1, width)


def solution(mesh):
    in_specs = (P("ctx", "head", None), P("ctx", "head", None), P("ctx", "head", None), P())
    out_specs = P("ctx", "head", None)
    body = functools.partial(local, mesh.shape["ctx"])
    return jax.shard_map(body, mesh=mesh, in_specs=in_specs, out_specs=out_specs, check_vma=False)
```
